32 devices in a mesh: ctx: 16 (over z, y, core), tp: 2 (over x).
Axes of the slice: x: 2, y: 2, z: 4, core: 2. Of those that a mesh axis runs over, the one named last changes fastest.
Arguments:
- queries: bfloat16 [2048, 8192], P('ctx', 'tp'), may hold values from -256 to 256
- keys: bfloat16 [2048, 1024], P(('ctx', 'tp')), may hold values from -6.5 to 6.5
- values: bfloat16 [2048, 1024], P(('ctx', 'tp')), may hold values from -6 to 6
- output_gradient: bfloat16 [2048, 8192], P('ctx', 'tp'), may hold values from -6 to 6
- span_order: int32 [32], replicated, may hold values from 0 to 31, as said below
Outputs:
- query_grad: bfloat16 [2048, 8192], P('ctx', 'tp')
- key_gradient_rows: bfloat16 [2048, 1024], P(('ctx', 'tp'))
- value_gradient_rows: bfloat16 [2048, 1024], P(('ctx', 'tp'))
The draws below stay inside these ranges and needn't reach their ends.
Inputs may be any that keep to these rules, and one draw needn't show every extreme that they name: `span_order`: each value 0 to 31 appears once; entries 2d and 2d + 1 sum to 31.
All inputs are finite; a program needn't handle non-finite values.
Results may differ from the reference program's by a relative error of at most 0.0073.
Values may be sent and summed in bfloat16 or wider, within the bound.
A program may use at most 64 MiB of HBM per device.

```python
import jax
import jax.numpy as jnp
from jax import lax

HEAD_SIZE = 128
QUERY_HEADS = 64
KEY_VALUE_HEADS = 8
TOK_DEV = 128
SPAN = 64
SEQUENCE_TOKENS = 2048


def joint_sample(key):
    base = jax.random.fold_in(key, 7)
    first_half, second = jax.random.split(base, 2)
    key_value_pairs = jnp.clip(jax.random.normal(first_half, (SEQUENCE_TOKENS, KEY_VALUE_HEADS, HEAD_SIZE), jnp.float32), -6.0, 6.0)
    query_vals = jnp.clip(jax.random.normal(second, (SEQUENCE_TOKENS, QUERY_HEADS, HEAD_SIZE), jnp.float32), -6.0, 6.0)
    query_vals = jnp.clip(query_vals, -256.0, 256.0)
    return (query_vals, key_value_pairs)


def draw_queries(key, part):
    return joint_sample(key)[0].reshape(SEQUENCE_TOKENS, QUERY_HEADS * HEAD_SIZE).astype(jnp.bfloat16)


def draw_keys(key, part):
    return joint_sample(key)[1].reshape(SEQUENCE_TOKENS, KEY_VALUE_HEADS * HEAD_SIZE).astype(jnp.bfloat16)


def draw_span_order(key, part):
    pairs = SEQUENCE_TOKENS // TOK_DEV
    perm = jax.random.permutation(jax.random.fold_in(key, 11), pairs).astype(jnp.int32)
    flips = jax.random.randint(jax.random.fold_in(key, 13), (pairs,), 0, 2)
    leading = jnp.where(flips == 0, perm, 2 * pairs - 1 - perm)
    trailing = 2 * pairs - 1 - leading
    return jnp.stack([leading, trailing], axis=1).reshape(-1).astype(jnp.int32)


def block_levels(key, dims, pieces, least, top_value):
    loudness, own = 1.0, jax.random.fold_in(key, 6)
    for axis_at, parts in pieces:
        steps = jnp.exp(jax.random.uniform(jax.random.fold_in(own, axis_at), (parts,), jnp.float32, least / len(pieces), top_value / len(pieces)))
        loudness = loudness * jnp.repeat(steps, dims[axis_at] // parts).reshape([-1 if axis == axis_at else 1 for axis in range(len(dims))])
    return loudness


def gaussian(key, shape, deviation, bound, cuts=(), kind=jnp.bfloat16):
    gain = block_levels(key, shape, cuts, -0.22, 0.18) if cuts else 1.0
    values = jax.random.normal(key, shape, jnp.float32) * deviation * gain
    return jnp.minimum(jnp.maximum(values, -bound), bound).astype(kind)


def setup_inputs(seed: int = 0) -> dict:
    key_of = jax.random.split(jax.random.key(seed), 6)
    queries = draw_queries(jax.random.fold_in(key_of[5], 71), 0)
    keys = draw_keys(jax.random.fold_in(key_of[5], 71), 0)
    values = gaussian(key_of[2], (SEQUENCE_TOKENS, KEY_VALUE_HEADS * HEAD_SIZE), 1.0, 6.0, ((0, 32),))
    output_gradient = gaussian(key_of[3], (SEQUENCE_TOKENS, QUERY_HEADS * HEAD_SIZE), 1.0, 6.0, ((0, 16), (1, 2)))
    span_order = draw_span_order(jax.random.fold_in(key_of[5], 71), 0)
    return dict(queries=queries, keys=keys, values=values, output_gradient=output_gradient, span_order=span_order)


def reference(queries, keys, values, output_gradient, span_order):
    scale = HEAD_SIZE ** -0.5
    head_group = QUERY_HEADS // KEY_VALUE_HEADS
    rows = jnp.arange(SEQUENCE_TOKENS, dtype=jnp.int32)
    pos = span_order[rows // SPAN] * SPAN + rows % SPAN
    visible = pos[:, None] >= pos[None, :]
    query_head_rows = queries.reshape(SEQUENCE_TOKENS, KEY_VALUE_HEADS, head_group, HEAD_SIZE).transpose(1, 2, 0, 3)
    gradient_heads = output_gradient.reshape(SEQUENCE_TOKENS, KEY_VALUE_HEADS, head_group, HEAD_SIZE).transpose(1, 2, 0, 3)
    key_head_rows = keys.reshape(SEQUENCE_TOKENS, KEY_VALUE_HEADS, HEAD_SIZE).transpose(1, 0, 2)
    value_head_rows = values.reshape(SEQUENCE_TOKENS, KEY_VALUE_HEADS, HEAD_SIZE).transpose(1, 0, 2)

    def one_group(items):
        q_group, g_group, k_group, v_group = items

        def one_head(carry, pair):
            q_head, g_head = pair
            score = jnp.dot(q_head, k_group.T, preferred_element_type=jnp.float32) * scale
            score = jnp.where(visible, score, -jnp.inf)
            top = jnp.max(score, axis=1, keepdims=True)
            expo = jnp.exp(score - top)
            prob = expo / jnp.sum(expo, axis=1, keepdims=True)
            dprob = jnp.dot(g_head, v_group.T, preferred_element_type=jnp.float32)
            delta = jnp.sum(prob * dprob, axis=1, keepdims=True)
            dscore = (prob * (dprob - delta) * scale).astype(jnp.bfloat16)
            weights = prob.astype(jnp.bfloat16)
            dquery = jnp.dot(dscore, k_group, preferred_element_type=jnp.float32)
            key_gradient = carry[0] + jnp.dot(dscore.T, q_head, preferred_element_type=jnp.float32)
            value_gradient = carry[1] + jnp.dot(weights.T, g_head, preferred_element_type=jnp.float32)
            return (key_gradient, value_gradient), dquery

        zeros = jnp.zeros((SEQUENCE_TOKENS, HEAD_SIZE), jnp.float32)
        (key_gradient, value_gradient), dquery = lax.scan(one_head, (zeros, zeros), (q_group, g_group))
        return dquery, key_gradient, value_gradient

    dquery, key_gradient, value_gradient = lax.map(one_group, (query_head_rows, gradient_heads, key_head_rows, value_head_rows))
    query_grad = dquery.transpose(2, 0, 1, 3).reshape(SEQUENCE_TOKENS, QUERY_HEADS * HEAD_SIZE).astype(jnp.bfloat16)
    key_gradient_rows = key_gradient.transpose(1, 0, 2).reshape(SEQUENCE_TOKENS, KEY_VALUE_HEADS * HEAD_SIZE).astype(jnp.bfloat16)
    value_gradient_rows = value_gradient.transpose(1, 0, 2).reshape(SEQUENCE_TOKENS, KEY_VALUE_HEADS * HEAD_SIZE).astype(jnp.bfloat16)
    return query_grad, key_gradient_rows, value_gradient_rows
```

```python
import functools
import math

import jax
import jax.numpy as jnp
from jax import lax
from jax.experimental import pallas as pl
from jax.experimental.pallas import tpu as pltpu
from jax.sharding import PartitionSpec as P

HEAD_SIZE = 128
QUERY_HEADS = 64
KEY_VALUE_HEADS = 8
GROUP = QUERY_HEADS // KEY_VALUE_HEADS
SCALE = HEAD_SIZE ** (-0.5)
LOG2E = math.log2(math.e)
NT = (((1,), (1,)), ((), ()))
F32 = jnp.float32
BF16 = jnp.bfloat16


def attention_kernel(
    order_ref, q_ref, g_ref, k_ref, v_ref, dq_ref, dk_ref, dv_ref,
    qs, gs, kseq, vseq, kt, s_buf, dp_buf, dk_acc, dv_acc, dq_acc, top, total, weighted,
    *, span, wide,
):
    spans = order_ref.shape[0]
    rows = GROUP * span
    width = wide * span
    tiles = spans // wide + 1
    me = lax.axis_index("ctx")
    first = order_ref[2 * me]
    second = order_ref[2 * me + 1]
    low_half = jnp.where(first < second, 0, 1)
    low = jnp.minimum(first, second)
    high = jnp.maximum(first, second)
    low_tiles = low // wide + 1

    for half in range(2):
        for h in range(GROUP):
            dst = pl.ds(h * span, span)
            src = (pl.ds(half * span, span), pl.ds(h * HEAD_SIZE, HEAD_SIZE))
            qs[half, dst, :] = q_ref[src]
            gs[half, dst, :] = g_ref[src]

    def place(b, _):
        src = pl.ds(pl.multiple_of(b * span, span), span)
        dst = pl.ds(pl.multiple_of(order_ref[b] * span, span), span)
        kseq[dst, :] = k_ref[src, :]
        vseq[dst, :] = v_ref[src, :]
        return 0

    lax.fori_loop(0, spans, place, 0)
    for b in range(spans // wide):
        kt[b] = kseq[pl.ds(b * width, width), :].T

    top[...] = jnp.full_like(top, -1e30)
    total[...] = jnp.zeros_like(total)
    weighted[...] = jnp.zeros_like(weighted)
    dq_acc[...] = jnp.zeros_like(dq_acc)
    dk_acc[...] = jnp.zeros_like(dk_acc)
    dv_acc[...] = jnp.zeros_like(dv_acc)

    def where(t):
        is_low = t < low_tiles
        half = jnp.where(is_low, low_half, 1 - low_half)
        block = jnp.where(is_low, t, t - low_tiles)
        last = jnp.logical_or(t == low_tiles - 1, t == tiles - 1)
        q_span = jnp.where(is_low, low, high)
        return half, block, last, q_span

    def keys_of(ref, block):
        return ref[pl.ds(pl.multiple_of(block * width, width), width), :]

    def score_step(t, _):
        half, block, last, q_span = where(t)
        s_buf[t] = lax.dot_general(
            keys_of(kseq, block), qs[half], NT, preferred_element_type=F32
        )

        @pl.when(last)
        def _():
            key_pos = block * width + lax.broadcasted_iota(jnp.int32, (width, rows), 0)
            q_pos = q_span * span + lax.broadcasted_iota(jnp.int32, (width, rows), 1) % span
            s_buf[t] = jnp.where(key_pos <= q_pos, s_buf[t], -1e30)

        part = jnp.max(s_buf[t].reshape(width // 8, 8, rows), axis=0)
        top[half] = jnp.maximum(top[half], part)
        return 0

    lax.fori_loop(0, tiles, score_step, 0)
    for half in range(2):
        top[half] = jnp.broadcast_to(jnp.max(top[half], axis=0, keepdims=True), (8, rows))

    def exp_step(t, _):
        half, block, _, _ = where(t)
        dp = lax.dot_general(keys_of(vseq, block), gs[half], NT, preferred_element_type=F32)
        e = jnp.exp2((s_buf[t] - top[half][0:1]) * (SCALE * LOG2E))
        s_buf[t] = e
        dp_buf[t] = dp
        total[half] += jnp.sum(e.reshape(width // 8, 8, rows), axis=0)
        weighted[half] += jnp.sum((e * dp).reshape(width // 8, 8, rows), axis=0)
        return 0

    lax.fori_loop(0, tiles, exp_step, 0)
    for half in range(2):
        inverse = 1.0 / jnp.sum(total[half], axis=0, keepdims=True)
        delta = jnp.sum(weighted[half], axis=0, keepdims=True) * inverse
        total[half] = jnp.broadcast_to(inverse, (8, rows))
        weighted[half] = jnp.broadcast_to(delta, (8, rows))

    def grad_step(t, _):
        half, block, _, _ = where(t)
        prob = s_buf[t] * total[half][0:1]
        dscore = (prob * (dp_buf[t] - weighted[half][0:1])).astype(BF16)
        weights = prob.astype(BF16)
        here = pl.ds(pl.multiple_of(block * width, width), width)
        dv_acc[here, :] += jnp.dot(weights, gs[half], preferred_element_type=F32)
        dk_acc[here, :] += jnp.dot(dscore, qs[half], preferred_element_type=F32)
        dq_acc[half] += jnp.dot(kt[block], dscore, preferred_element_type=F32)
        return 0

    lax.fori_loop(0, tiles, grad_step, 0)

    for half in range(2):
        dq = (dq_acc[half] * SCALE).T.astype(BF16)
        for h in range(GROUP):
            dq_ref[pl.ds(half * span, span), pl.ds(h * HEAD_SIZE, HEAD_SIZE)] = dq[
                h * span : (h + 1) * span
            ]

    def put(b, _):
        dst = pl.ds(pl.multiple_of(b * span, span), span)
        src = pl.ds(pl.multiple_of(order_ref[b] * span, span), span)
        dk_ref[dst, :] = (dk_acc[src, :] * SCALE).astype(dk_ref.dtype)
        dv_ref[dst, :] = dv_acc[src, :].astype(dv_ref.dtype)
        return 0

    lax.fori_loop(0, spans, put, 0)


def attention(order, q, g, kv, kv_heads, grad_type):
    tokens, length = q.shape[0], kv.shape[0]
    spans = order.shape[0]
    span = tokens // 2
    rows = GROUP * span
    wide = math.gcd(spans, 4)
    width = wide * span
    tiles = spans // wide + 1
    d = HEAD_SIZE
    elements = kv_heads * tiles * width * rows
    smem = pl.BlockSpec(memory_space=pltpu.SMEM)
    head_block = pl.BlockSpec((tokens, GROUP * d), lambda i: (0, i))
    return pl.pallas_call(
        functools.partial(attention_kernel, span=span, wide=wide),
        grid=(kv_heads,),
        in_specs=[
            smem,
            head_block,
            head_block,
            pl.BlockSpec((length, d), lambda i: (0, i)),
            pl.BlockSpec((length, d), lambda i: (0, i + kv_heads)),
        ],
        out_specs=[
            head_block,
            pl.BlockSpec((length, d), lambda i: (0, i)),
            pl.BlockSpec((length, d), lambda i: (0, i)),
        ],
        out_shape=[
            jax.ShapeDtypeStruct(q.shape, BF16),
            jax.ShapeDtypeStruct((length, kv_heads * d), grad_type),
            jax.ShapeDtypeStruct((length, kv_heads * d), grad_type),
        ],
        scratch_shapes=[
            pltpu.VMEM((2, rows, d), BF16),
            pltpu.VMEM((2, rows, d), BF16),
            pltpu.VMEM((length, d), BF16),
            pltpu.VMEM((length, d), BF16),
            pltpu.VMEM((spans // wide, d, width), BF16),
            pltpu.VMEM((tiles, width, rows), F32),
            pltpu.VMEM((tiles, width, rows), F32),
            pltpu.VMEM((length, d), F32),
            pltpu.VMEM((length, d), F32),
            pltpu.VMEM((2, d, rows), F32),
            pltpu.VMEM((2, 8, rows), F32),
            pltpu.VMEM((2, 8, rows), F32),
            pltpu.VMEM((2, 8, rows), F32),
        ],
        compiler_params=pltpu.CompilerParams(vmem_limit_bytes=48 * 2**20),
        cost_estimate=pl.CostEstimate(
            flops=10 * elements * d, bytes_accessed=8 * 2**20, transcendentals=elements
        ),
        name="attention_grad",
    )(order, q, g, kv, kv)


def body(queries, keys, values, output_gradient, span_order):
    tp = lax.axis_size("tp")
    local = keys.shape[0]
    mine = keys.shape[1] // tp
    kv_heads = mine // HEAD_SIZE
    pair = jnp.stack(
        [keys.reshape(local, tp, mine), values.reshape(local, tp, mine)], axis=2
    ).reshape(local, tp * 2 * mine)
    pair = lax.all_to_all(pair, "tp", split_axis=1, concat_axis=0, tiled=True)
    whole = lax.all_gather(pair, "ctx", axis=0, tiled=True)
    dq, dk, dv = attention(span_order, queries, output_gradient, whole, kv_heads, F32)
    dk = lax.psum_scatter(dk, "ctx", scatter_dimension=0, tiled=True).astype(BF16)
    dv = lax.psum_scatter(dv, "ctx", scatter_dimension=0, tiled=True).astype(BF16)
    both = lax.all_to_all(
        jnp.stack([dk, dv], axis=1), "tp", split_axis=0, concat_axis=2, tiled=True
    )
    return dq, both[:, 0], both[:, 1]


def solution(mesh):
    return jax.shard_map(
        body,
        mesh=mesh,
        in_specs=(
            P("ctx", "tp"),
            P(("ctx", "tp"), None),
            P(("ctx", "tp"), None),
            P("ctx", "tp"),
            P(),
        ),
        out_specs=(P("ctx", "tp"), P(("ctx", "tp"), None), P(("ctx", "tp"), None)),
        check_vma=False,
    )
```

```python
import functools
import math

import jax
import jax.numpy as jnp
from jax import lax
from jax.experimental import pallas as pl
from jax.experimental.pallas import tpu as pltpu
from jax.sharding import PartitionSpec as P

HEAD_SIZE = 128
QUERY_HEADS = 64
KEY_VALUE_HEADS = 8
GROUP = QUERY_HEADS // KEY_VALUE_HEADS
SCALE = HEAD_SIZE ** (-0.5)
LOG2E = math.log2(math.e)
PIECES = 4
NT = (((1,), (1,)), ((), ()))
F32 = jnp.float32
BF16 = jnp.bfloat16


def attention_kernel(
    order_ref, q_ref, g_ref, k_ref, v_ref, dq_ref, out_ref,
    qs, gs, kseq, vseq, kt, s_buf, dp_buf, dk_acc, dv_acc, dq_acc, top, total, weighted,
    *, span, wide,
):
    spans = order_ref.shape[0]
    rows = GROUP * span
    width = wide * span
    tiles = spans // wide + 1
    me = lax.axis_index("ctx")
    first = order_ref[2 * me]
    second = order_ref[2 * me + 1]
    low_half = jnp.where(first < second, 0, 1)
    low = jnp.minimum(first, second)
    high = jnp.maximum(first, second)
    low_tiles = low // wide + 1

    for half in range(2):
        for h in range(GROUP):
            dst = pl.ds(h * span, span)
            src = (pl.ds(half * span, span), pl.ds(h * HEAD_SIZE, HEAD_SIZE))
            qs[half, dst, :] = q_ref[src]
            gs[half, dst, :] = g_ref[src]

    def place(b, _):
        src = pl.ds(pl.multiple_of(b * span, span), span)
        dst = pl.ds(pl.multiple_of(order_ref[b] * span, span), span)
        kseq[dst, :] = k_ref[src, :]
        vseq[dst, :] = v_ref[src, :]
        return 0

    lax.fori_loop(0, spans, place, 0)
    for b in range(spans // wide):
        kt[b] = kseq[pl.ds(b * width, width), :].T

    top[...] = jnp.full_like(top, -1e30)
    total[...] = jnp.zeros_like(total)
    weighted[...] = jnp.zeros_like(weighted)
    dq_acc[...] = jnp.zeros_like(dq_acc)
    dk_acc[...] = jnp.zeros_like(dk_acc)
    dv_acc[...] = jnp.zeros_like(dv_acc)

    def where(t):
        is_low = t < low_tiles
        half = jnp.where(is_low, low_half, 1 - low_half)
        block = jnp.where(is_low, t, t - low_tiles)
        last = jnp.logical_or(t == low_tiles - 1, t == tiles - 1)
        q_span = jnp.where(is_low, low, high)
        return half, block, last, q_span

    def keys_of(ref, block):
        return ref[pl.ds(pl.multiple_of(block * width, width), width), :]

    def score_step(t, _):
        half, block, last, q_span = where(t)
        s_buf[t] = lax.dot_general(
            keys_of(kseq, block), qs[half], NT, preferred_element_type=F32
        )

        @pl.when(last)
        def _():
            key_pos = block * width + lax.broadcasted_iota(jnp.int32, (width, rows), 0)
            q_pos = q_span * span + lax.broadcasted_iota(jnp.int32, (width, rows), 1) % span
            s_buf[t] = jnp.where(key_pos <= q_pos, s_buf[t], -1e30)

        part = jnp.max(s_buf[t].reshape(width // 8, 8, rows), axis=0)
        top[half] = jnp.maximum(top[half], part)
        return 0

    lax.fori_loop(0, tiles, score_step, 0)
    for half in range(2):
        top[half] = jnp.broadcast_to(jnp.max(top[half], axis=0, keepdims=True), (8, rows))

    def exp_step(t, _):
        half, block, _, _ = where(t)
        dp = lax.dot_general(keys_of(vseq, block), gs[half], NT, preferred_element_type=F32)
        e = jnp.exp2((s_buf[t] - top[half][0:1]) * (SCALE * LOG2E))
        s_buf[t] = e
        dp_buf[t] = dp
        total[half] += jnp.sum(e.reshape(width // 8, 8, rows), axis=0)
        weighted[half] += jnp.sum((e * dp).reshape(width // 8, 8, rows), axis=0)
        return 0

    lax.fori_loop(0, tiles, exp_step, 0)
    for half in range(2):
        inverse = 1.0 / jnp.sum(total[half], axis=0, keepdims=True)
        delta = jnp.sum(weighted[half], axis=0, keepdims=True) * inverse
        total[half] = jnp.broadcast_to(inverse, (8, rows))
        weighted[half] = jnp.broadcast_to(delta, (8, rows))

    def grad_step(t, _):
        half, block, _, _ = where(t)
        prob = s_buf[t] * total[half][0:1]
        dscore = (prob * (dp_buf[t] - weighted[half][0:1])).astype(BF16)
        weights = prob.astype(BF16)
        here = pl.ds(pl.multiple_of(block * width, width), width)
        dv_acc[here, :] += jnp.dot(weights, gs[half], preferred_element_type=F32)
        dk_acc[here, :] += jnp.dot(dscore, qs[half], preferred_element_type=F32)
        dq_acc[half] += jnp.dot(kt[block], dscore, preferred_element_type=F32)
        return 0

    lax.fori_loop(0, tiles, grad_step, 0)

    for half in range(2):
        dq = (dq_acc[half] * SCALE).T.astype(BF16)
        for h in range(GROUP):
            dq_ref[pl.ds(half * span, span), pl.ds(h * HEAD_SIZE, HEAD_SIZE)] = dq[
                h * span : (h + 1) * span
            ]

    def put(b, _):
        dst = pl.ds(pl.multiple_of(b * span, span), span)
        src = pl.ds(pl.multiple_of(order_ref[b] * span, span), span)
        out_ref[0, dst, :] = (dk_acc[src, :] * SCALE).astype(BF16)
        out_ref[1, dst, :] = dv_acc[src, :].astype(BF16)
        return 0

    lax.fori_loop(0, spans, put, 0)


def attention(order, q, g, kv):
    tokens, length = q.shape[0], kv.shape[1]
    kv_heads = kv.shape[2] // HEAD_SIZE
    spans = order.shape[0]
    span = tokens // 2
    rows = GROUP * span
    wide = math.gcd(spans, 4)
    width = wide * span
    tiles = spans // wide + 1
    d = HEAD_SIZE
    elements = kv_heads * tiles * width * rows
    smem = pl.BlockSpec(memory_space=pltpu.SMEM)
    head_block = pl.BlockSpec((tokens, GROUP * d), lambda i: (0, i))
    return pl.pallas_call(
        functools.partial(attention_kernel, span=span, wide=wide),
        grid=(kv_heads,),
        in_specs=[
            smem,
            head_block,
            head_block,
            pl.BlockSpec((None, length, d), lambda i: (0, 0, i)),
            pl.BlockSpec((None, length, d), lambda i: (1, 0, i)),
        ],
        out_specs=[
            head_block,
            pl.BlockSpec((2, length, d), lambda i: (0, 0, i)),
        ],
        out_shape=[
            jax.ShapeDtypeStruct(q.shape, BF16),
            jax.ShapeDtypeStruct(kv.shape, BF16),
        ],
        scratch_shapes=[
            pltpu.VMEM((2, rows, d), BF16),
            pltpu.VMEM((2, rows, d), BF16),
            pltpu.VMEM((length, d), BF16),
            pltpu.VMEM((length, d), BF16),
            pltpu.VMEM((spans // wide, d, width), BF16),
            pltpu.VMEM((tiles, width, rows), F32),
            pltpu.VMEM((tiles, width, rows), F32),
            pltpu.VMEM((length, d), F32),
            pltpu.VMEM((length, d), F32),
            pltpu.VMEM((2, d, rows), F32),
            pltpu.VMEM((2, 8, rows), F32),
            pltpu.VMEM((2, 8, rows), F32),
            pltpu.VMEM((2, 8, rows), F32),
        ],
        compiler_params=pltpu.CompilerParams(vmem_limit_bytes=48 * 2**20),
        cost_estimate=pl.CostEstimate(
            flops=10 * elements * d, bytes_accessed=8 * 2**20, transcendentals=elements
        ),
        name="attention_grad",
    )(order, q, g, kv, kv)


def ring_place(chips):
    ctx = lax.axis_index("ctx")
    chip, core = ctx // 2, ctx % 2
    depth, column = chip // 2, chip % 2
    return chip, core, (1 - column) * depth + column * (chips - 1 - depth)


def chip_at(position, chips):
    column = position // (chips // 2)
    depth = (1 - column) * position + column * (chips - 1 - position)
    return 2 * depth + column


def device(ctx, tp):
    return dict(device_id=(ctx, tp), device_id_type=pl.DeviceIdType.MESH)


def greet(targets):
    barrier = pltpu.get_barrier_semaphore()
    for target in targets:
        pl.semaphore_signal(barrier, inc=1, **target)
    pl.semaphore_wait(barrier, len(targets))


def pieces_of(rows):
    return math.gcd(rows // 2, PIECES)


def gather_kernel(
    keys_ref, values_ref, out_ref,
    tp_send, tp_recv, own_sem, pair_send, pair_recv, ring_send, ring_recv, side_send, side_recv,
    *, chips, tp_size,
):
    local, mine = keys_ref.shape[0], out_ref.shape[2]
    tokens = local * tp_size
    block = 2 * tokens
    pieces = pieces_of(block)
    piece = block // pieces
    chip, core, position = ring_place(chips)
    ctx, tp = lax.axis_index("ctx"), lax.axis_index("tp")
    way = 1 - 2 * core
    partner = device(2 * chip + 1 - core, tp)
    ahead = device(2 * chip_at((position + way + chips) % chips, chips) + core, tp)
    behind = device(2 * chip_at((position - way + chips) % chips, chips) + core, tp)
    others = [(tp + i) % tp_size for i in range(1, tp_size)]
    greet([partner, ahead, behind] + [device(ctx, t) for t in others])

    def at(start, size):
        return pl.ds(pl.multiple_of(start, size), size)

    sources = (keys_ref, values_ref)
    copies = []
    landed = at(ctx * tokens + tp * local, local)
    for a in range(2):
        for i, t in enumerate(others):
            copies.append(
                pltpu.make_async_remote_copy(
                    src_ref=sources[a].at[:, at(t * mine, mine)],
                    dst_ref=out_ref.at[a, landed],
                    send_sem=tp_send.at[a, i],
                    recv_sem=tp_recv.at[a, i],
                    **device(ctx, t),
                )
            )
            copies[-1].start()
    own = []
    for a in range(2):
        own.append(
            pltpu.make_async_copy(
                sources[a].at[:, at(tp * mine, mine)], out_ref.at[a, landed], own_sem.at[a]
            )
        )
        own[-1].start()
    for copy in own:
        copy.wait()
    for copy in copies:
        copy.wait()

    pair = []
    for a in range(2):
        rows = out_ref.at[a, at(ctx * tokens, tokens)]
        pair.append(
            pltpu.make_async_remote_copy(
                src_ref=rows, dst_ref=rows,
                send_sem=pair_send.at[a], recv_sem=pair_recv.at[a], **partner,
            )
        )
        pair[-1].start()
    for copy in pair:
        copy.wait()

    def ring_copy(step, j):
        origin = chip_at((position - way * step + 2 * chips * chips) % chips, chips)
        rows = out_ref.at[core, at(origin * block + j * piece, piece)]
        return pltpu.make_async_remote_copy(
            src_ref=rows, dst_ref=rows,
            send_sem=ring_send.at[step, j], recv_sem=ring_recv.at[step, j], **ahead,
        )

    def side_copy(step, j):
        origin = chip_at((position - way * step + 2 * chips * chips) % chips, chips)
        rows = out_ref.at[core, at(origin * block + j * piece, piece)]
        return pltpu.make_async_remote_copy(
            src_ref=rows, dst_ref=rows,
            send_sem=side_send.at[step - 1, j], recv_sem=side_recv.at[step - 1, j], **partner,
        )

    for j in range(pieces):
        ring_copy(0, j).start()

    def forward(step, _):
        for j in range(pieces):
            ring_copy(step - 1, j).wait_recv()
            ring_copy(step, j).start()
            side_copy(step, j).start()
        return 0

    lax.fori_loop(1, chips - 1, forward, 0)
    for j in range(pieces):
        ring_copy(chips - 2, j).wait_recv()
        side_copy(chips - 1, j).start()

    def finish(step, _):
        for j in range(pieces):
            ring_copy(step - 1, j).wait_send()
            side_copy(step, j).wait()
        return 0

    lax.fori_loop(1, chips, finish, 0)


def gather(keys, values, ctx_size, tp_size):
    local, mine = keys.shape[0], keys.shape[1] // tp_size
    length = local * tp_size * ctx_size
    chips = ctx_size // 2
    pieces = pieces_of(2 * local * tp_size)
    dma = pltpu.SemaphoreType.DMA
    vmem = pl.BlockSpec(memory_space=pltpu.VMEM)
    return pl.pallas_call(
        functools.partial(gather_kernel, chips=chips, tp_size=tp_size),
        in_specs=[vmem, vmem],
        out_specs=vmem,
        out_shape=jax.ShapeDtypeStruct((2, length, mine), BF16),
        scratch_shapes=[
            dma((2, tp_size - 1)), dma((2, tp_size - 1)), dma((2,)), dma((2,)), dma((2,)),
            dma((chips - 1, pieces)), dma((chips - 1, pieces)),
            dma((chips - 1, pieces)), dma((chips - 1, pieces)),
        ],
        compiler_params=pltpu.CompilerParams(collective_id=0, has_side_effects=True),
        name="gather_pairs",
    )(keys, values)


def scatter_kernel(
    grads_ref, out_ref, pair_buf, ring_in, ring_out, final,
    pair_send, pair_recv, ring_send, ring_recv, last_send, last_recv, own_sem,
    *, chips, tp_size,
):
    mine = grads_ref.shape[2]
    block = grads_ref.shape[1] // chips
    tokens = block // 2
    local = tokens // tp_size
    pieces = pieces_of(block)
    piece = block // pieces
    chip, core, position = ring_place(chips)
    tp = lax.axis_index("tp")
    way = 1 - 2 * core
    partner = device(2 * chip + 1 - core, tp)
    ahead = device(2 * chip_at((position + way + chips) % chips, chips) + core, tp)
    behind = device(2 * chip_at((position - way + chips) % chips, chips) + core, tp)
    owners = [
        (other, (tp + i) % tp_size, other * tp_size + i)
        for other in range(2)
        for i in range(tp_size)
    ]
    remote = owners[1:]
    greet(
        [partner, ahead, behind]
        + [device(2 * chip + (core + o) % 2, t) for o, t, _ in remote]
    )

    def at(start, size):
        return pl.ds(pl.multiple_of(start, size), size)

    def target(step, sign):
        return chip_at((position - sign * (1 + step) + 2 * chips * chips) % chips, chips)

    def pair_copy(step, j):
        rows = at(target(step, -way) * block + j * piece, piece)
        return pltpu.make_async_remote_copy(
            src_ref=grads_ref.at[1 - core, rows],
            dst_ref=pair_buf.at[step, at(j * piece, piece)],
            send_sem=pair_send.at[step, j], recv_sem=pair_recv.at[step, j], **partner,
        )

    def ring_copy(step, j):
        rows = at(j * piece, piece)
        return pltpu.make_async_remote_copy(
            src_ref=ring_out.at[step, rows],
            dst_ref=ring_in.at[step, rows],
            send_sem=ring_send.at[step, j], recv_sem=ring_recv.at[step, j], **ahead,
        )

    def start_pairs(step, _):
        for j in range(pieces):
            pair_copy(step, j).start()
        return 0

    lax.fori_loop(0, chips, start_pairs, 0)

    def local_terms(step, j):
        pair_copy(step, j).wait_recv()
        rows = at(target(step, way) * block + j * piece, piece)
        theirs = pair_buf[step, pl.ds(j * piece, piece), :].astype(F32)
        return grads_ref[core, rows, :].astype(F32) + theirs

    for j in range(pieces):
        ring_out[0, pl.ds(j * piece, piece), :] = local_terms(0, j).astype(BF16)
        ring_copy(0, j).start()

    def step_body(step, _):
        for j in range(pieces):
            terms = local_terms(step, j)
            ring_copy(step - 1, j).wait_recv()
            rows = pl.ds(j * piece, piece)
            arrived = ring_in[step - 1, rows, :].astype(F32)
            ring_out[step, rows, :] = (terms + arrived).astype(BF16)
            ring_copy(step, j).start()
        return 0

    lax.fori_loop(1, chips - 1, step_body, 0)
    for j in range(pieces):
        terms = local_terms(chips - 1, j)
        ring_copy(chips - 2, j).wait_recv()
        rows = pl.ds(j * piece, piece)
        final[rows, :] = (terms + ring_in[chips - 2, rows, :].astype(F32)).astype(BF16)

    columns = at(tp * mine, mine)
    last = []
    for o, t, sem in remote:
        who = (core + o) % 2
        last.append(
            pltpu.make_async_remote_copy(
                src_ref=final.at[at(who * tokens + t * local, local)],
                dst_ref=out_ref.at[core, :, columns],
                send_sem=last_send.at[sem], recv_sem=last_recv.at[sem],
                **device(2 * chip + who, t),
            )
        )
        last[-1].start()
    own = pltpu.make_async_copy(
        final.at[at(core * tokens + tp * local, local)], out_ref.at[core, :, columns], own_sem
    )
    own.start()
    own.wait()
    for copy in last:
        copy.wait()

    def finish(step, _):
        for j in range(pieces):
            ring_copy(step, j).wait_send()
            pair_copy(step, j).wait_send()
        return 0

    lax.fori_loop(0, chips - 1, finish, 0)
    for j in range(pieces):
        pair_copy(chips - 1, j).wait_send()


def scatter(grads, ctx_size, tp_size):
    _, length, mine = grads.shape
    chips = ctx_size // 2
    block = length // chips
    local = block // 2 // tp_size
    pieces = pieces_of(block)
    dma = pltpu.SemaphoreType.DMA
    vmem = pl.BlockSpec(memory_space=pltpu.VMEM)
    return pl.pallas_call(
        functools.partial(scatter_kernel, chips=chips, tp_size=tp_size),
        in_specs=[vmem],
        out_specs=vmem,
        out_shape=jax.ShapeDtypeStruct((2, local, mine * tp_size), BF16),
        scratch_shapes=[
            pltpu.VMEM((chips, block, mine), BF16),
            pltpu.VMEM((chips - 1, block, mine), BF16),
            pltpu.VMEM((chips - 1, block, mine), BF16),
            pltpu.VMEM((block, mine), BF16),
            dma((chips, pieces)), dma((chips, pieces)),
            dma((chips - 1, pieces)), dma((chips - 1, pieces)),
            dma((2 * tp_size,)), dma((2 * tp_size,)), dma,
        ],
        compiler_params=pltpu.CompilerParams(collective_id=1, has_side_effects=True),
        name="scatter_pairs",
    )(grads)


def body(queries, keys, values, output_gradient, span_order):
    ctx_size, tp_size = lax.axis_size("ctx"), lax.axis_size("tp")
    kv = gather(keys, values, ctx_size, tp_size)
    dq, grads = attention(span_order, queries, output_gradient, kv)
    both = scatter(grads, ctx_size, tp_size)
    return dq, both[0], both[1]


def solution(mesh):
    return jax.shard_map(
        body,
        mesh=mesh,
        in_specs=(
            P("ctx", "tp"),
            P(("ctx", "tp"), None),
            P(("ctx", "tp"), None),
            P("ctx", "tp"),
            P(),
        ),
        out_specs=(P("ctx", "tp"), P(("ctx", "tp"), None), P(("ctx", "tp"), None)),
        check_vma=False,
    )
```

```python
import functools
import math

import jax
import jax.numpy as jnp
from jax import lax
from jax.experimental import pallas as pl
from jax.experimental.pallas import tpu as pltpu
from jax.sharding import PartitionSpec as P

HEAD_SIZE = 128
QUERY_HEADS = 64
KEY_VALUE_HEADS = 8
GROUP = QUERY_HEADS // KEY_VALUE_HEADS
SCALE = HEAD_SIZE ** (-0.5)
LOG2E = math.log2(math.e)
PIECES = 8
UNROLL = 9
NT = (((1,), (1,)), ((), ()))
F32 = jnp.float32
BF16 = jnp.bfloat16


def attention_kernel(
    order_ref, q_ref, g_ref, k_ref, v_ref, dq_ref, out_ref,
    qs, gs, kseq, vseq, kt, s_buf, dp_buf, dk_acc, dv_acc, dq_acc, top, total, weighted,
    *, span, wide,
):
    spans = order_ref.shape[0]
    rows = GROUP * span
    width = wide * span
    tiles = spans // wide + 1
    me = lax.axis_index("ctx")
    first = order_ref[2 * me]
    second = order_ref[2 * me + 1]
    low_half = jnp.where(first < second, 0, 1)
    low = jnp.minimum(first, second)
    high = jnp.maximum(first, second)
    low_tiles = low // wide + 1

    for half in range(2):
        for h in range(GROUP):
            dst = pl.ds(h * span, span)
            src = (pl.ds(half * span, span), pl.ds(h * HEAD_SIZE, HEAD_SIZE))
            qs[half, dst, :] = q_ref[src]
            gs[half, dst, :] = g_ref[src]

    def place(b, _):
        src = pl.ds(pl.multiple_of(b * span, span), span)
        dst = pl.ds(pl.multiple_of(order_ref[b] * span, span), span)
        kseq[dst, :] = k_ref[src, :]
        vseq[dst, :] = v_ref[src, :]
        return 0

    lax.fori_loop(0, spans, place, 0)
    for b in range(spans // wide):
        kt[b] = kseq[pl.ds(b * width, width), :].T

    top[...] = jnp.full_like(top, -1e30)
    total[...] = jnp.zeros_like(total)
    weighted[...] = jnp.zeros_like(weighted)
    dq_acc[...] = jnp.zeros_like(dq_acc)
    dk_acc[...] = jnp.zeros_like(dk_acc)
    dv_acc[...] = jnp.zeros_like(dv_acc)

    def where(t):
        is_low = t < low_tiles
        half = jnp.where(is_low, low_half, 1 - low_half)
        block = jnp.where(is_low, t, t - low_tiles)
        last = jnp.logical_or(t == low_tiles - 1, t == tiles - 1)
        q_span = jnp.where(is_low, low, high)
        return half, block, last, q_span

    def keys_of(ref, block):
        return ref[pl.ds(pl.multiple_of(block * width, width), width), :]

    def sweep(step):
        def several(i, _):
            for u in range(UNROLL):
                step(i * UNROLL + u)
            return 0

        lax.fori_loop(0, tiles // UNROLL, several, 0)
        for t in range(tiles // UNROLL * UNROLL, tiles):
            step(t)

    def raise_top(half, score, skip):
        part = jnp.max(score.reshape(width // 8, 8, rows), axis=0)
        top[half] = jnp.maximum(top[half], jnp.where(skip, -1e30, part))

    def score_step(t):
        half, block, last, _ = where(t)
        score = lax.dot_general(keys_of(kseq, block), qs[half], NT, preferred_element_type=F32)
        s_buf[t] = score
        raise_top(half, score, last)

    sweep(score_step)
    for t in (low_tiles - 1, tiles - 1):
        half, block, _, q_span = where(t)
        key_pos = block * width + lax.broadcasted_iota(jnp.int32, (width, rows), 0)
        q_pos = q_span * span + lax.broadcasted_iota(jnp.int32, (width, rows), 1) % span
        score = jnp.where(key_pos <= q_pos, s_buf[t], -1e30)
        s_buf[t] = score
        raise_top(half, score, False)
    for half in range(2):
        top[half] = jnp.broadcast_to(jnp.max(top[half], axis=0, keepdims=True), (8, rows))

    def exp_step(t):
        half, block, _, _ = where(t)
        dp = lax.dot_general(keys_of(vseq, block), gs[half], NT, preferred_element_type=F32)
        e = jnp.exp2((s_buf[t] - top[half][0:1]) * (SCALE * LOG2E))
        s_buf[t] = e
        dp_buf[t] = dp
        total[half] += jnp.sum(e.reshape(width // 8, 8, rows), axis=0)
        weighted[half] += jnp.sum((e * dp).reshape(width // 8, 8, rows), axis=0)

    sweep(exp_step)
    for half in range(2):
        inverse = 1.0 / jnp.sum(total[half], axis=0, keepdims=True)
        delta = jnp.sum(weighted[half], axis=0, keepdims=True) * inverse
        total[half] = jnp.broadcast_to(inverse, (8, rows))
        weighted[half] = jnp.broadcast_to(delta, (8, rows))

    def grad_step(t):
        half, block, _, _ = where(t)
        prob = s_buf[t] * total[half][0:1]
        dscore = (prob * (dp_buf[t] - weighted[half][0:1])).astype(BF16)
        weights = prob.astype(BF16)
        here = pl.ds(pl.multiple_of(block * width, width), width)
        dv_acc[here, :] += jnp.dot(weights, gs[half], preferred_element_type=F32)
        dk_acc[here, :] += jnp.dot(dscore, qs[half], preferred_element_type=F32)
        dq_acc[half] += jnp.dot(kt[block], dscore, preferred_element_type=F32)

    sweep(grad_step)

    for half in range(2):
        dq = (dq_acc[half] * SCALE).T.astype(BF16)
        for h in range(GROUP):
            dq_ref[pl.ds(half * span, span), pl.ds(h * HEAD_SIZE, HEAD_SIZE)] = dq[
                h * span : (h + 1) * span
            ]

    def put(b, _):
        dst = pl.ds(pl.multiple_of(b * span, span), span)
        src = pl.ds(pl.multiple_of(order_ref[b] * span, span), span)
        out_ref[0, dst, :] = (dk_acc[src, :] * SCALE).astype(BF16)
        out_ref[1, dst, :] = dv_acc[src, :].astype(BF16)
        return 0

    lax.fori_loop(0, spans, put, 0)


def attention(order, q, g, kv):
    tokens, length = q.shape[0], kv.shape[1]
    kv_heads = kv.shape[2] // HEAD_SIZE
    spans = order.shape[0]
    span = tokens // 2
    rows = GROUP * span
    wide = math.gcd(spans, 4)
    width = wide * span
    tiles = spans // wide + 1
    d = HEAD_SIZE
    elements = kv_heads * tiles * width * rows
    smem = pl.BlockSpec(memory_space=pltpu.SMEM)
    head_block = pl.BlockSpec((tokens, GROUP * d), lambda i: (0, i))
    return pl.pallas_call(
        functools.partial(attention_kernel, span=span, wide=wide),
        grid=(kv_heads,),
        in_specs=[
            smem,
            head_block,
            head_block,
            pl.BlockSpec((None, length, d), lambda i: (0, 0, i)),
            pl.BlockSpec((None, length, d), lambda i: (1, 0, i)),
        ],
        out_specs=[
            head_block,
            pl.BlockSpec((2, length, d), lambda i: (0, 0, i)),
        ],
        out_shape=[
            jax.ShapeDtypeStruct(q.shape, BF16),
            jax.ShapeDtypeStruct(kv.shape, BF16),
        ],
        scratch_shapes=[
            pltpu.VMEM((2, rows, d), BF16),
            pltpu.VMEM((2, rows, d), BF16),
            pltpu.VMEM((length, d), BF16),
            pltpu.VMEM((length, d), BF16),
            pltpu.VMEM((spans // wide, d, width), BF16),
            pltpu.VMEM((tiles, width, rows), F32),
            pltpu.VMEM((tiles, width, rows), F32),
            pltpu.VMEM((length, d), F32),
            pltpu.VMEM((length, d), F32),
            pltpu.VMEM((2, d, rows), F32),
            pltpu.VMEM((2, 8, rows), F32),
            pltpu.VMEM((2, 8, rows), F32),
            pltpu.VMEM((2, 8, rows), F32),
        ],
        compiler_params=pltpu.CompilerParams(vmem_limit_bytes=48 * 2**20),
        cost_estimate=pl.CostEstimate(
            flops=10 * elements * d, bytes_accessed=8 * 2**20, transcendentals=elements
        ),
        name="attention_grad",
    )(order, q, g, kv, kv)


def ring_place(chips):
    ctx = lax.axis_index("ctx")
    chip, core = ctx // 2, ctx % 2
    depth, column = chip // 2, chip % 2
    return chip, core, (1 - column) * depth + column * (chips - 1 - depth)


def chip_at(position, chips):
    column = position // (chips // 2)
    depth = (1 - column) * position + column * (chips - 1 - position)
    return 2 * depth + column


def device(ctx, tp):
    return dict(device_id=(ctx, tp), device_id_type=pl.DeviceIdType.MESH)


def greet(targets):
    barrier = pltpu.get_barrier_semaphore()
    for target in targets:
        pl.semaphore_signal(barrier, inc=1, **target)
    pl.semaphore_wait(barrier, len(targets))


def pieces_of(rows):
    return math.gcd(rows // 2, PIECES)


def gather_kernel(
    keys_ref, values_ref, out_ref,
    tp_send, tp_recv, own_sem, pair_send, pair_recv, ring_send, ring_recv, side_send, side_recv,
    *, chips, tp_size,
):
    local, mine = keys_ref.shape[0], out_ref.shape[2]
    tokens = local * tp_size
    block = 2 * tokens
    pieces = pieces_of(block)
    piece = block // pieces
    chip, core, position = ring_place(chips)
    ctx, tp = lax.axis_index("ctx"), lax.axis_index("tp")
    way = 1 - 2 * core
    partner = device(2 * chip + 1 - core, tp)
    ahead = device(2 * chip_at((position + way + chips) % chips, chips) + core, tp)
    behind = device(2 * chip_at((position - way + chips) % chips, chips) + core, tp)
    others = [(tp + i) % tp_size for i in range(1, tp_size)]
    greet([partner, ahead, behind] + [device(ctx, t) for t in others])

    def at(start, size):
        return pl.ds(pl.multiple_of(start, size), size)

    sources = (keys_ref, values_ref)
    copies = []
    landed = at(ctx * tokens + tp * local, local)
    for a in range(2):
        for i, t in enumerate(others):
            copies.append(
                pltpu.make_async_remote_copy(
                    src_ref=sources[a].at[:, at(t * mine, mine)],
                    dst_ref=out_ref.at[a, landed],
                    send_sem=tp_send.at[a, i],
                    recv_sem=tp_recv.at[a, i],
                    **device(ctx, t),
                )
            )
            copies[-1].start()
    own = []
    for a in range(2):
        own.append(
            pltpu.make_async_copy(
                sources[a].at[:, at(tp * mine, mine)], out_ref.at[a, landed], own_sem.at[a]
            )
        )
        own[-1].start()
    half = pieces // 2
    early = local // piece if local % piece == 0 else 0

    def rows_of(step, j):
        origin = chip_at((position - way * step + 2 * chips * chips) % chips, chips)
        inside = ((tp * local) // piece * piece + (j % half) * piece) % tokens
        return at(origin * block + ((core + j // half) % 2) * tokens + inside, piece)

    def ring_copy(step, j):
        rows = out_ref.at[core, rows_of(step, j)]
        return pltpu.make_async_remote_copy(
            src_ref=rows, dst_ref=rows,
            send_sem=ring_send.at[step, j], recv_sem=ring_recv.at[step, j], **ahead,
        )

    def side_copy(step, j):
        rows = out_ref.at[core, rows_of(step, j)]
        return pltpu.make_async_remote_copy(
            src_ref=rows, dst_ref=rows,
            send_sem=side_send.at[step - 1, j], recv_sem=side_recv.at[step - 1, j], **partner,
        )

    for copy in own:
        copy.wait()
    for j in range(early):
        ring_copy(0, j).start()
    for copy in copies:
        copy.wait()
    for j in range(early, half):
        ring_copy(0, j).start()

    pair = []
    for a in range(2):
        rows = out_ref.at[a, at(ctx * tokens, tokens)]
        pair.append(
            pltpu.make_async_remote_copy(
                src_ref=rows, dst_ref=rows,
                send_sem=pair_send.at[a], recv_sem=pair_recv.at[a], **partner,
            )
        )
        pair[-1].start()
    for copy in pair:
        copy.wait()
    for j in range(half, pieces):
        ring_copy(0, j).start()

    def forward(step, _):
        for j in range(pieces):
            ring_copy(step - 1, j).wait_recv()
            ring_copy(step, j).start()
            side_copy(step, j).start()
        return 0

    lax.fori_loop(1, chips - 1, forward, 0)
    for j in range(pieces):
        ring_copy(chips - 2, j).wait_recv()
        side_copy(chips - 1, j).start()

    def finish(step, _):
        for j in range(pieces):
            ring_copy(step - 1, j).wait_send()
            side_copy(step, j).wait()
        return 0

    lax.fori_loop(1, chips, finish, 0)


def gather(keys, values, ctx_size, tp_size):
    local, mine = keys.shape[0], keys.shape[1] // tp_size
    length = local * tp_size * ctx_size
    chips = ctx_size // 2
    pieces = pieces_of(2 * local * tp_size)
    dma = pltpu.SemaphoreType.DMA
    vmem = pl.BlockSpec(memory_space=pltpu.VMEM)
    return pl.pallas_call(
        functools.partial(gather_kernel, chips=chips, tp_size=tp_size),
        in_specs=[vmem, vmem],
        out_specs=vmem,
        out_shape=jax.ShapeDtypeStruct((2, length, mine), BF16),
        scratch_shapes=[
            dma((2, tp_size - 1)), dma((2, tp_size - 1)), dma((2,)), dma((2,)), dma((2,)),
            dma((chips - 1, pieces)), dma((chips - 1, pieces)),
            dma((chips - 1, pieces)), dma((chips - 1, pieces)),
        ],
        compiler_params=pltpu.CompilerParams(collective_id=0, has_side_effects=True),
        name="gather_pairs",
    )(keys, values)


def scatter_kernel(
    grads_ref, out_ref, pair_buf, ring_in, ring_out, final,
    pair_send, pair_recv, ring_send, ring_recv, last_send, last_recv, own_sem,
    *, chips, tp_size,
):
    mine = grads_ref.shape[2]
    block = grads_ref.shape[1] // chips
    tokens = block // 2
    local = tokens // tp_size
    pieces = pieces_of(block)
    piece = block // pieces
    chip, core, position = ring_place(chips)
    tp = lax.axis_index("tp")
    way = 1 - 2 * core
    partner = device(2 * chip + 1 - core, tp)
    ahead = device(2 * chip_at((position + way + chips) % chips, chips) + core, tp)
    behind = device(2 * chip_at((position - way + chips) % chips, chips) + core, tp)
    owners = [
        (other, (tp + i) % tp_size, other * tp_size + i)
        for other in range(2)
        for i in range(tp_size)
    ]
    remote = owners[1:]
    greet(
        [partner, ahead, behind]
        + [device(2 * chip + (core + o) % 2, t) for o, t, _ in remote]
    )

    def at(start, size):
        return pl.ds(pl.multiple_of(start, size), size)

    def target(step, sign):
        return chip_at((position - sign * (1 + step) + 2 * chips * chips) % chips, chips)

    def pair_copy(step, j):
        rows = at(target(step, -way) * block + j * piece, piece)
        return pltpu.make_async_remote_copy(
            src_ref=grads_ref.at[1 - core, rows],
            dst_ref=pair_buf.at[step, at(j * piece, piece)],
            send_sem=pair_send.at[step, j], recv_sem=pair_recv.at[step, j], **partner,
        )

    def ring_copy(step, j):
        rows = at(j * piece, piece)
        return pltpu.make_async_remote_copy(
            src_ref=ring_out.at[step, rows],
            dst_ref=ring_in.at[step, rows],
            send_sem=ring_send.at[step, j], recv_sem=ring_recv.at[step, j], **ahead,
        )

    def start_pairs(step, _):
        for j in range(pieces):
            pair_copy(step, j).start()
        return 0

    lax.fori_loop(0, chips, start_pairs, 0)

    def local_terms(step, j):
        pair_copy(step, j).wait_recv()
        rows = at(target(step, way) * block + j * piece, piece)
        theirs = pair_buf[step, pl.ds(j * piece, piece), :].astype(F32)
        return grads_ref[core, rows, :].astype(F32) + theirs

    for j in range(pieces):
        ring_out[0, pl.ds(j * piece, piece), :] = local_terms(0, j).astype(BF16)
        ring_copy(0, j).start()

    def step_body(step, _):
        for j in range(pieces):
            terms = local_terms(step, j)
            ring_copy(step - 1, j).wait_recv()
            rows = pl.ds(j * piece, piece)
            arrived = ring_in[step - 1, rows, :].astype(F32)
            ring_out[step, rows, :] = (terms + arrived).astype(BF16)
            ring_copy(step, j).start()
        return 0

    lax.fori_loop(1, chips - 1, step_body, 0)
    for j in range(pieces):
        terms = local_terms(chips - 1, j)
        ring_copy(chips - 2, j).wait_recv()
        rows = pl.ds(j * piece, piece)
        final[rows, :] = (terms + ring_in[chips - 2, rows, :].astype(F32)).astype(BF16)

    columns = at(tp * mine, mine)
    last = []
    for o, t, sem in remote:
        who = (core + o) % 2
        last.append(
            pltpu.make_async_remote_copy(
                src_ref=final.at[at(who * tokens + t * local, local)],
                dst_ref=out_ref.at[core, :, columns],
                send_sem=last_send.at[sem], recv_sem=last_recv.at[sem],
                **device(2 * chip + who, t),
            )
        )
        last[-1].start()
    own = pltpu.make_async_copy(
        final.at[at(core * tokens + tp * local, local)], out_ref.at[core, :, columns], own_sem
    )
    own.start()
    own.wait()
    for copy in last:
        copy.wait()

    def finish(step, _):
        for j in range(pieces):
            ring_copy(step, j).wait_send()
            pair_copy(step, j).wait_send()
        return 0

    lax.fori_loop(0, chips - 1, finish, 0)
    for j in range(pieces):
        pair_copy(chips - 1, j).wait_send()


def scatter(grads, ctx_size, tp_size):
    _, length, mine = grads.shape
    chips = ctx_size // 2
    block = length // chips
    local = block // 2 // tp_size
    pieces = pieces_of(block)
    dma = pltpu.SemaphoreType.DMA
    vmem = pl.BlockSpec(memory_space=pltpu.VMEM)
    return pl.pallas_call(
        functools.partial(scatter_kernel, chips=chips, tp_size=tp_size),
        in_specs=[vmem],
        out_specs=vmem,
        out_shape=jax.ShapeDtypeStruct((2, local, mine * tp_size), BF16),
        scratch_shapes=[
            pltpu.VMEM((chips, block, mine), BF16),
            pltpu.VMEM((chips - 1, block, mine), BF16),
            pltpu.VMEM((chips - 1, block, mine), BF16),
            pltpu.VMEM((block, mine), BF16),
            dma((chips, pieces)), dma((chips, pieces)),
            dma((chips - 1, pieces)), dma((chips - 1, pieces)),
            dma((2 * tp_size,)), dma((2 * tp_size,)), dma,
        ],
        compiler_params=pltpu.CompilerParams(collective_id=1, has_side_effects=True),
        name="scatter_pairs",
    )(grads)


def body(queries, keys, values, output_gradient, span_order):
    ctx_size, tp_size = lax.axis_size("ctx"), lax.axis_size("tp")
    kv = gather(keys, values, ctx_size, tp_size)
    dq, grads = attention(span_order, queries, output_gradient, kv)
    both = scatter(grads, ctx_size, tp_size)
    return dq, both[0], both[1]


def solution(mesh):
    return jax.shard_map(
        body,
        mesh=mesh,
        in_specs=(
            P("ctx", "tp"),
            P(("ctx", "tp"), None),
            P(("ctx", "tp"), None),
            P("ctx", "tp"),
            P(),
        ),
        out_specs=(P("ctx", "tp"), P(("ctx", "tp"), None), P(("ctx", "tp"), None)),
        check_vma=False,
    )
```
